32 devices in a mesh: dp: 8 (over z, core), fsdp: 4 (over y, x).
Axes of the slice: x: 2, y: 2, z: 4, core: 2. Of those that a mesh axis runs over, the one named last changes fastest.
Arguments:
- logits: bfloat16 [4096, 32000], P('dp', 'fsdp'), may hold values from -115 to 125
- labels: int32 [4096], P('dp'), may hold values from 0 to 31999
- activations: bfloat16 [4096, 5120], P('dp', 'fsdp'), may hold values from -6 to 6
- proj_in: bfloat16 [5120, 64], P('fsdp'), may hold values from -0.078125 to 0.078125
- proj_out: bfloat16 [32000, 64], P('fsdp'), may hold values from -6 to 6
Outputs:
- features: float32 [512, 4096], P(('dp', 'fsdp'))
- gram: float32 [4096, 4096], P('fsdp', 'dp')
The draws below stay inside these ranges and needn't reach their ends.
All inputs are finite; a program needn't handle non-finite values.
Results may differ from the reference program's by a relative error of at most 0.014.
Values may be sent and summed in bfloat16 or wider, within the bound.
No kernel may reach another device: no remote copies, remote signals or barrier semaphores. Data moves between devices by JAX's collectives and lax.ppermute only.
A program may use at most 64 MiB of HBM per device.

```python
import jax
import jax.numpy as jnp
from jax import lax

D = 5120
V = 32000
K_IN = 64
K_OUT = 64
SEQ = 8
EX_DEV = 64
FEAT = 4096
EXAMPLES = 512
TOKENS = 4096
N_DP = 8


def draw_logits(key, part):
    first = jax.random.fold_in(jax.random.fold_in(key, 11), 0)
    base = jnp.clip(3.0 * jax.random.normal(first, (TOKENS, V), jnp.float32), -15.0, 15.0)
    return base.astype(jnp.bfloat16)


def set_ends(values, rng, least, top_value):
    longest = values.shape.index(max(values.shape))
    spots = []
    for shift in (0, 1):
        where = [jax.random.randint(jax.random.fold_in(rng, axis), (), 0, length) for axis, length in enumerate(values.shape)]
        where[longest] = (where[longest] + shift) % values.shape[longest]
        spots.append(tuple(where))
    return values.at[spots[0]].set(least).at[spots[1]].set(top_value)


def steps_of(own_key, dims, cuts, smallest, top_value):
    gain = 1.0
    for position, shards_of in cuts:
        steps = jax.random.uniform(jax.random.fold_in(jax.random.fold_in(own_key, 6), position), (shards_of,), jnp.float32, smallest / len(cuts), top_value / len(cuts))
        gain = gain * jnp.repeat(jnp.exp(steps), dims[position] // shards_of).reshape((-1,) + (1,) * (len(dims) - 1 - position))
    return gain


def gaussian(key, dims, scale, reach, shards=(), kind=jnp.bfloat16):
    drawn = scale * jax.random.normal(key, dims, jnp.float32)
    if shards:
        drawn = drawn * steps_of(key, dims, shards, -0.22, 0.18)
    return jnp.clip(drawn, -reach, reach).astype(kind)


def setup_inputs(seed: int = 0) -> dict:
    seeds = jax.random.split(jax.random.key(seed), 6)
    logits = draw_logits(jax.random.fold_in(seeds[5], 71), 0)
    labels = set_ends(jax.random.randint(seeds[1], (TOKENS,), 0, V), jax.random.fold_in(seeds[1], 1), 0, V - 1).astype(jnp.int32)
    activations = gaussian(seeds[2], (TOKENS, D), 1.0, 6.0, ((0, 8), (1, 4)))
    proj_in = gaussian(seeds[3], (D, K_IN), D ** -0.5, 0.078125, ((0, 4),))
    proj_out = gaussian(seeds[4], (V, K_OUT), 1.0, 6.0, ((0, 4),))
    return {"logits": logits, "labels": labels, "activations": activations, "proj_in": proj_in, "proj_out": proj_out}


def reference(logits, labels, activations, proj_in, proj_out):
    tok_dev = EX_DEV * SEQ
    blocks_logits = logits.reshape(N_DP, tok_dev, V)
    blocks_labels = labels.reshape(N_DP, tok_dev)
    blocks_act = activations.reshape(N_DP, tok_dev, D)

    def one_block(items):
        block_logits, block_labels, block_act = items
        values = block_logits.astype(jnp.float32)
        top = jnp.max(values, axis=1, keepdims=True)
        expo = jnp.exp(values - top)
        prob = expo / jnp.sum(expo, axis=1, keepdims=True)
        columns = lax.broadcasted_iota(jnp.int32, (1, V), 1)
        onehot = (columns == block_labels[:, None]).astype(jnp.float32)
        errors = (prob - onehot).astype(jnp.bfloat16)
        left = jnp.dot(block_act, proj_in, preferred_element_type=jnp.float32)
        right = jnp.dot(errors, proj_out, preferred_element_type=jnp.float32)
        sketch = jnp.einsum("esi,esj->eij", left.reshape(EX_DEV, SEQ, K_IN), right.reshape(EX_DEV, SEQ, K_OUT))
        return sketch.reshape(EX_DEV, K_IN * K_OUT)

    features = lax.map(one_block, (blocks_logits, blocks_labels, blocks_act)).reshape(EXAMPLES, FEAT)
    rounded = features.astype(jnp.bfloat16)
    gram = jnp.dot(rounded.T, rounded, preferred_element_type=jnp.float32)
    return features, gram
```

```python
import functools

import jax
import jax.numpy as jnp
from jax import lax
from jax.experimental import pallas as pl
from jax.experimental.pallas import tpu as pltpu
from jax.sharding import PartitionSpec as P

SEQ = 8
LOG2E = 1.4426950408889634
LANES = 128
CHUNK = 1024
SUB = 256
STAT = 16
F32 = jnp.float32
BF16 = jnp.bfloat16


def _cdiv(a, b):
    return (a + b - 1) // b


def _sizes(total, step):
    out = []
    start = 0
    while start < total:
        out.append((start, min(step, total - start)))
        start += step
    return out


def _local_kernel(
    logits_hbm, labels_hbm, act_hbm, pin_hbm, pout_hbm, *rest, groups, vocab, tokens, width, k_in, k_out
):
    outs = rest[:groups]
    buf, lab, act, pin, pext, acc, plab, top, msg, sem, lsem = rest[groups:]
    copies = [
        pltpu.make_async_copy(pin_hbm, pin, sem.at[0]),
        pltpu.make_async_copy(act_hbm, act, sem.at[1]),
        pltpu.make_async_copy(pout_hbm, pext.at[0:k_out, :], sem.at[2]),
        pltpu.make_async_copy(labels_hbm, lab, sem.at[3]),
    ]
    for c in copies:
        c.start()
    chunks = _sizes(vocab, CHUNK)
    loads = []
    for n, (start, size) in enumerate(chunks):
        c = pltpu.make_async_copy(logits_hbm.at[start : start + size, :], buf.at[start : start + size, :], lsem.at[n])
        c.start()
        loads.append(c)
    mine = lax.axis_index("fsdp")
    copies[0].wait()
    copies[1].wait()
    left = lax.dot_general(pin[...], act[...], (((1,), (1,)), ((), ())), preferred_element_type=F32)
    msg[0:k_in, :] = left.astype(BF16)
    copies[2].wait()
    copies[3].wait()
    pext[k_out : k_out + STAT, :] = jnp.ones((STAT, vocab), BF16)
    acc[...] = jnp.zeros_like(acc)
    plab[...] = jnp.zeros_like(plab)
    top[...] = jnp.full_like(top, -1e30)
    local = lab[...] - mine * vocab
    inside = (local >= 0) & (local < vocab)
    local = jnp.where(inside, local, -LANES)
    block = lax.shift_right_arithmetic(local, 7)
    lane = jnp.bitwise_and(local, LANES - 1)

    for n, (start, size) in enumerate(chunks):
        loads[n].wait()
        peak = None
        for r, h in _sizes(size, 16):
            part = buf[start + r : start + r + h, :]
            peak = part if peak is None else jnp.maximum(peak, part)
        peak = jnp.max(peak.astype(F32), axis=0, keepdims=True)
        old = top[...]
        new = jnp.maximum(old, peak)
        top[...] = new
        keep = jnp.exp2((old - new) * LOG2E)
        total = acc[...] * keep
        for r, h in _sizes(size, SUB):
            part = buf[start + r : start + r + h, :].astype(F32)
            expo = jnp.exp2((part - new) * LOG2E).astype(BF16)
            total = total + jnp.dot(pext[:, start + r : start + r + h], expo, preferred_element_type=F32)
        acc[...] = total
        for t in range(_cdiv(tokens, LANES)):
            cols = slice(t * LANES, (t + 1) * LANES)
            which = jnp.broadcast_to(block[:, cols], (k_out, LANES))
            index = jnp.broadcast_to(lane[:, cols], (k_out, LANES))
            found = plab[:, cols]
            for r, h in _sizes(size, LANES):
                tile = pext[0:k_out, start + r : start + r + h].astype(F32)
                if h < LANES:
                    tile = jnp.concatenate([tile, jnp.zeros((k_out, LANES - h), F32)], axis=1)
                got = jnp.take_along_axis(tile, index, axis=1)
                found = jnp.where(which == (start + r) // LANES, got, found)
            plab[:, cols] = found

    msg[k_in : k_in + k_out, :] = acc[0:k_out, :].astype(BF16)
    msg[k_in + k_out : k_in + 2 * k_out, :] = plab[...].astype(BF16)
    sums = acc[k_out : k_out + STAT, :]
    high = sums.astype(BF16).astype(F32)
    row = lax.broadcasted_iota(jnp.int32, (STAT, tokens), 0)
    stat = jnp.where(row == 0, top[...], jnp.where(row == 1, high, jnp.where(row == 2, sums - high, 0.0)))
    msg[k_in + 2 * k_out :, :] = stat.astype(BF16)
    share = tokens // groups
    examples = tokens // SEQ
    src = lax.broadcasted_iota(jnp.int32, (tokens, tokens), 0)
    dst = lax.broadcasted_iota(jnp.int32, (tokens, tokens), 1) + mine * share
    dst = jnp.where(dst >= tokens, dst - tokens, dst)
    want = jnp.bitwise_and(dst, examples - 1) * SEQ + lax.shift_right_arithmetic(dst, examples.bit_length() - 1)
    moved = jnp.dot(msg[...], jnp.where(src == want, 1.0, 0.0).astype(BF16), preferred_element_type=F32).astype(BF16)
    for k in range(groups):
        outs[k][...] = moved[:, k * share : (k + 1) * share]


def _local(logits, labels, act, pin, pout, groups):
    vocab, tokens = logits.shape
    k_in, width = pin.shape
    k_out = pout.shape[0]
    rows = k_in + 2 * k_out + STAT
    share = tokens // groups
    n_chunks = _cdiv(vocab, CHUNK)
    any_spec = pl.BlockSpec(memory_space=pl.ANY)
    return pl.pallas_call(
        functools.partial(
            _local_kernel, groups=groups, vocab=vocab, tokens=tokens, width=width, k_in=k_in, k_out=k_out
        ),
        out_shape=[jax.ShapeDtypeStruct((rows, share), BF16)] * groups,
        in_specs=[any_spec] * 5,
        out_specs=[pl.BlockSpec(memory_space=pltpu.VMEM)] * groups,
        scratch_shapes=[
            pltpu.VMEM((vocab, tokens), BF16),
            pltpu.VMEM((1, tokens), jnp.int32),
            pltpu.VMEM((tokens, width), BF16),
            pltpu.VMEM((k_in, width), BF16),
            pltpu.VMEM((k_out + STAT, vocab), BF16),
            pltpu.VMEM((k_out + STAT, tokens), F32),
            pltpu.VMEM((k_out, tokens), F32),
            pltpu.VMEM((1, tokens), F32),
            pltpu.VMEM((rows, tokens), BF16),
            pltpu.SemaphoreType.DMA((4,)),
            pltpu.SemaphoreType.DMA((n_chunks,)),
        ],
        name="local_pass",
    )(logits, labels, act, pin, pout)


def _join_kernel(*refs, k_in, k_out):
    parts, out = refs[:-1], refs[-1]
    base = k_in + 2 * k_out
    stats = [p[base : base + STAT, :].astype(F32) for p in parts]
    top = functools.reduce(jnp.maximum, [s[0:1] for s in stats])
    weights = [jnp.exp2((s[0:1] - top) * LOG2E) for s in stats]
    total = sum(w * (s[1:2] + s[2:3]) for w, s in zip(weights, stats))
    scale = 1.0 / total
    left = sum(p[0:k_in, :].astype(F32) for p in parts)
    right = sum(p[k_in : k_in + k_out, :].astype(F32) * w for p, w in zip(parts, weights)) * scale
    right = right - sum(p[k_in + k_out : base, :].astype(F32) for p in parts)
    out[0:k_in, :] = left.astype(BF16)
    out[k_in : k_in + k_out, :] = right.astype(BF16)


def _join(parts, k_in, k_out):
    return pl.pallas_call(
        functools.partial(_join_kernel, k_in=k_in, k_out=k_out),
        out_shape=jax.ShapeDtypeStruct((k_in + k_out, parts[0].shape[1]), BF16),
        in_specs=[pl.BlockSpec(memory_space=pltpu.VMEM)] * len(parts),
        out_specs=pl.BlockSpec(memory_space=pltpu.VMEM),
        name="join",
    )(*parts)


def _gram_body(x, out_hbm, frow, fcol, res, sem, n_row, n_col, k_out):
    lanes = x.shape[2]
    base = n_row + n_col

    def feature_rows(first, count, dest, dest_first):
        for z in range(lanes // LANES):
            cols = slice(z * LANES, (z + 1) * LANES)
            for j in range(0, k_out, 16):
                rights = [x[t, base + j : base + j + 16, cols] for t in range(SEQ)]
                for i in range(count):
                    total = None
                    for t in range(SEQ):
                        term = x[t, first + i : first + i + 1, cols] * rights[t]
                        total = term if total is None else total + term
                    at = dest_first + i * k_out + j
                    dest[at : at + 16, cols] = total.astype(BF16)

    feature_rows(n_row, n_col, fcol, 0)
    step = max(1, n_row // 4)
    copies = []
    for b, i in enumerate(range(0, n_row, step)):
        feature_rows(i, step, frow, i * k_out)
        rows = slice(i * k_out, (i + step) * k_out)
        res[rows, :] = lax.dot_general(
            frow[rows, :], fcol[...], (((1,), (1,)), ((), ())), preferred_element_type=F32
        )
        c = pltpu.make_async_copy(res.at[rows, :], out_hbm.at[rows, :], sem.at[b])
        c.start()
        copies.append(c)
    for c in copies:
        c.wait()


def _gram_kernel(*refs, n_in, blocks, examples, n_row, n_col, k_in, k_out):
    ins, out_hbm = refs[:n_in], refs[n_in]
    x, frow, fcol, res, sem = refs[n_in + 1 :]
    rows = k_in + k_out
    half = n_in // 2
    if blocks:
        row_first = lax.axis_index("fsdp") * n_row
        col_first = lax.axis_index("dp") * n_col
        per = LANES // examples
        for k in range(half):
            for z in range(blocks):
                takes = [
                    (pl.ds(pl.multiple_of(z * rows + row_first, 8), n_row), 0, n_row),
                    (pl.ds(pl.multiple_of(z * rows + col_first, 8), n_col), n_row, n_col),
                    (slice(z * rows + k_in, (z + 1) * rows), n_row + n_col, k_out),
                ]
                for take, at, count in takes:
                    own = ins[k][take, :].astype(F32)
                    other = ins[half + k][take, :].astype(F32)
                    for s in range(per):
                        piece = slice(s * examples, (s + 1) * examples)
                        x[k * per + s, at : at + count, z * LANES : (z + 1) * LANES] = jnp.concatenate(
                            [own[:, piece], other[:, piece]], axis=1
                        )
    else:
        x[...] = ins[0][...].astype(F32)
    _gram_body(x, out_hbm, frow, fcol, res, sem, n_row, n_col, k_out)


def _gram(ins, blocks, examples, lanes, n_row, n_col, k_in, k_out):
    rows, cols = n_row * k_out, n_col * k_out
    return pl.pallas_call(
        functools.partial(
            _gram_kernel,
            n_in=len(ins),
            blocks=blocks,
            examples=examples,
            n_row=n_row,
            n_col=n_col,
            k_in=k_in,
            k_out=k_out,
        ),
        out_shape=jax.ShapeDtypeStruct((rows, cols), F32),
        in_specs=[pl.BlockSpec(memory_space=pltpu.VMEM)] * len(ins),
        out_specs=pl.BlockSpec(memory_space=pl.ANY),
        scratch_shapes=[
            pltpu.VMEM((SEQ, n_row + n_col + k_out, lanes), F32),
            pltpu.VMEM((rows, lanes), BF16),
            pltpu.VMEM((cols, lanes), BF16),
            pltpu.VMEM((rows, cols), F32),
            pltpu.SemaphoreType.DMA((8,)),
        ],
        name="gram",
    )(*ins)


def body(logits, labels, activations, proj_in, proj_out):
    n_f, n_d = lax.axis_size("fsdp"), lax.axis_size("dp")
    tokens = logits.shape[0]
    k_in, k_out = proj_in.shape[1], proj_out.shape[1]
    rows = k_in + k_out
    examples = tokens // SEQ
    own_examples = examples // n_f
    share = tokens // n_f

    def along_f(a, k):
        return lax.ppermute(a, "fsdp", [(i, (i + k) % n_f) for i in range(n_f)])

    def along_z(a, k):
        return lax.ppermute(a, "dp", [(i, (i + 2 * k) % n_d) for i in range(n_d)])

    def other_core(a):
        return lax.ppermute(a, "dp", [(i, i ^ 1) for i in range(n_d)])

    parts = _local(logits.T, labels.reshape(1, tokens), activations, proj_in.T, proj_out.T, n_f)
    parts = [parts[0]] + [along_f(parts[k], k) for k in range(1, n_f)]
    joined = _join(parts, k_in, k_out)
    n_z = n_d // 2
    column = jnp.concatenate([joined] + [along_z(joined, k) for k in range(1, n_z)], axis=0)
    own = [column] + [along_f(column, k) for k in range(1, n_f)]
    other = [other_core(a) for a in own]

    mine = lax.axis_index("fsdp")
    if share >= examples:
        slots = share // examples
        pieces = []
        for a in own:
            part = a[:rows].reshape(rows, slots, examples)
            pieces.append(lax.dynamic_slice_in_dim(part, mine * own_examples, own_examples, 2))
        group = jnp.concatenate(pieces, axis=1)
    else:
        order = [(mine - k) % n_f for k in range(n_f)]
        whole = jnp.zeros((n_f, rows, share), BF16)
        for k, a in enumerate(own):
            whole = lax.dynamic_update_slice(whole, a[:rows][None], (order[k], 0, 0))
        whole = whole.transpose(1, 0, 2).reshape(rows, SEQ, examples)
        group = lax.dynamic_slice_in_dim(whole, mine * own_examples, own_examples, 2)
    features = jnp.einsum("ite,jte->eij", group[:k_in], group[k_in:], preferred_element_type=F32)
    features = features.reshape(own_examples, k_in * k_out)

    n_row, n_col = k_in // n_f, k_in // n_d
    lanes = examples * n_d
    if share == LANES and 2 * examples == LANES and n_row % 8 == 0 and n_col % 8 == 0:
        gram = _gram(own + other, n_z, examples, lanes, n_row, n_col, k_in, k_out)
    else:
        order = [(mine - k) % n_f for k in range(n_f)]
        whole = jnp.zeros((n_f, 2, n_z, rows, share), BF16)
        for c, arrays in enumerate((own, other)):
            for k, a in enumerate(arrays):
                whole = lax.dynamic_update_slice(whole, a.reshape(1, 1, n_z, rows, share), (order[k], c, 0, 0, 0))
        whole = whole.transpose(3, 1, 2, 0, 4).reshape(rows, 2, n_z, SEQ, examples)
        whole = whole.transpose(3, 0, 1, 2, 4).reshape(SEQ, rows, lanes)
        whole = jnp.concatenate(
            [
                lax.dynamic_slice_in_dim(whole, mine * n_row, n_row, 1),
                lax.dynamic_slice_in_dim(whole, lax.axis_index("dp") * n_col, n_col, 1),
                whole[:, k_in:],
            ],
            axis=1,
        )
        gram = _gram([whole], 0, examples, lanes, n_row, n_col, k_in, k_out)
    return features, gram


def solution(mesh):
    in_specs = (P("dp", "fsdp"), P("dp"), P("dp", "fsdp"), P("fsdp", None), P("fsdp", None))
    out_specs = (P(("dp", "fsdp"), None), P("fsdp", "dp"))
    return jax.shard_map(body, mesh=mesh, in_specs=in_specs, out_specs=out_specs, check_vma=False)
```

```python
import functools

import jax
import jax.numpy as jnp
from jax import lax
from jax.experimental import pallas as pl
from jax.experimental.pallas import tpu as pltpu
from jax.sharding import PartitionSpec as P

SEQ = 8
LOG2E = 1.4426950408889634
LANES = 128
CHUNK = 3456
SUB = 256
STAT = 16
AHEAD = 20
FIRST = 1152
F32 = jnp.float32
BF16 = jnp.bfloat16


def _cdiv(a, b):
    return (a + b - 1) // b


def _sizes(total, step, first=None):
    out = []
    start = 0
    while start < total:
        size = min(first if first and not start else step, total - start)
        out.append((start, size))
        start += size
    return out


def _partner(i, k, n):
    return i ^ k if n & (n - 1) == 0 else (i + k) % n


def _on_chip(arrays):
    return [pltpu.with_memory_space_constraint(a, pltpu.VMEM) for a in arrays]


def _local_kernel(
    logits_hbm, labels_hbm, act_hbm, pin_hbm, pout_hbm, *rest, groups, vocab, tokens, width, k_in, k_out
):
    outs = rest[:groups]
    buf, lab, act, pin, pext, wide, acc, plab, top, msg, sem, lsem, psem = rest[groups:]
    chunks = _sizes(vocab, CHUNK, FIRST)
    queue, loads, pout_loads = [], [], []
    label_load = pltpu.make_async_copy(labels_hbm, lab, sem.at[0])
    act_load = pltpu.make_async_copy(act_hbm, act, sem.at[1])
    pin_load = pltpu.make_async_copy(pin_hbm, pin, sem.at[2])
    for n, (start, size) in enumerate(chunks):
        cols = slice(start, start + size)
        loads.append(pltpu.make_async_copy(logits_hbm.at[cols, :], buf.at[cols, :], lsem.at[n]))
        pout_loads.append(pltpu.make_async_copy(pout_hbm.at[:, cols], pext.at[0:k_out, cols], psem.at[n]))
        queue.append((loads[n], pout_loads[n], label_load) if n == 0 else (loads[n], pout_loads[n]))
        if n == min(3, len(chunks) - 1):
            queue.append((act_load, pin_load))
    started = 0

    def start_next(count):
        nonlocal started
        for group in queue[started : started + count]:
            for c in group:
                c.start()
        started += count

    start_next(AHEAD)
    mine = lax.axis_index("fsdp")
    label_load.wait()
    pext[k_out : k_out + STAT, :] = jnp.ones((STAT, vocab), BF16)
    acc[...] = jnp.zeros_like(acc)
    plab[...] = jnp.zeros_like(plab)
    top[...] = jnp.full_like(top, -1e30)
    local = lab[...] - mine * vocab
    inside = (local >= 0) & (local < vocab)
    local = jnp.where(inside, local, -LANES)
    block = lax.shift_right_arithmetic(local, 7)
    lane = jnp.bitwise_and(local, LANES - 1)

    for n, (start, size) in enumerate(chunks):
        loads[n].wait()
        pout_loads[n].wait()
        start_next(1)
        if n == min(2, len(chunks) - 1):
            start_next(len(queue))
            act_load.wait()
            pin_load.wait()
            left = lax.dot_general(pin[...], act[...], (((1,), (1,)), ((), ())), preferred_element_type=F32)
            msg[0:k_in, :] = left.astype(BF16)
        peak = None
        for r, h in _sizes(size, 16):
            part = buf[start + r : start + r + h, :]
            peak = part if peak is None else jnp.maximum(peak, part)
        peak = jnp.max(peak.astype(F32), axis=0, keepdims=True)
        old = top[...]
        new = jnp.maximum(old, peak)
        top[...] = new
        keep = jnp.exp2((old - new) * LOG2E)
        total = acc[...] * keep
        for r, h in _sizes(size, SUB):
            part = buf[start + r : start + r + h, :].astype(F32)
            expo = jnp.exp2((part - new) * LOG2E).astype(BF16)
            total = total + jnp.dot(pext[:, start + r : start + r + h], expo, preferred_element_type=F32)
        acc[...] = total
        blocks = _sizes(size, LANES)
        for r, h in blocks:
            wide[:, r : r + h] = pext[0:k_out, start + r : start + r + h].astype(F32)
        for t in range(_cdiv(tokens, LANES)):
            cols = slice(t * LANES, (t + 1) * LANES)
            which = jnp.broadcast_to(block[:, cols], (k_out, LANES))
            index = jnp.broadcast_to(lane[:, cols], (k_out, LANES))
            found = plab[:, cols]
            for r, h in blocks:
                got = jnp.take_along_axis(wide[:, r : r + LANES], index, axis=1)
                found = jnp.where(which == (start + r) // LANES, got, found)
            plab[:, cols] = found

    msg[k_in : k_in + k_out, :] = acc[0:k_out, :].astype(BF16)
    msg[k_in + k_out : k_in + 2 * k_out, :] = plab[...].astype(BF16)
    sums = acc[k_out : k_out + STAT, :]
    high = sums.astype(BF16).astype(F32)
    row = lax.broadcasted_iota(jnp.int32, (STAT, tokens), 0)
    stat = jnp.where(row == 0, top[...], jnp.where(row == 1, high, jnp.where(row == 2, sums - high, 0.0)))
    msg[k_in + 2 * k_out :, :] = stat.astype(BF16)
    share = tokens // groups
    examples = tokens // SEQ
    src = lax.broadcasted_iota(jnp.int32, (tokens, share), 0)
    place = lax.broadcasted_iota(jnp.int32, (tokens, share), 1)
    for k in range(groups):
        dst = place + _partner(mine, k, groups) * share
        want = jnp.bitwise_and(dst, examples - 1) * SEQ + lax.shift_right_arithmetic(dst, examples.bit_length() - 1)
        pick = jnp.where(src == want, 1.0, 0.0).astype(BF16)
        outs[k][...] = jnp.dot(msg[...], pick, preferred_element_type=F32).astype(BF16)


def _local(logits, labels, act, pin, pout, groups):
    vocab, tokens = logits.shape
    k_in, width = pin.shape
    k_out = pout.shape[0]
    rows = k_in + 2 * k_out + STAT
    share = tokens // groups
    n_chunks = len(_sizes(vocab, CHUNK, FIRST))
    any_spec = pl.BlockSpec(memory_space=pl.ANY)
    return pl.pallas_call(
        functools.partial(
            _local_kernel, groups=groups, vocab=vocab, tokens=tokens, width=width, k_in=k_in, k_out=k_out
        ),
        out_shape=[pltpu.VMEM((rows, share), BF16)] * groups,
        in_specs=[any_spec] * 5,
        out_specs=[pl.BlockSpec(memory_space=pltpu.VMEM)] * groups,
        scratch_shapes=[
            pltpu.VMEM((vocab, tokens), BF16),
            pltpu.VMEM((1, tokens), jnp.int32),
            pltpu.VMEM((tokens, width), BF16),
            pltpu.VMEM((k_in, width), BF16),
            pltpu.VMEM((k_out + STAT, vocab), BF16),
            pltpu.VMEM((k_out, CHUNK), F32),
            pltpu.VMEM((k_out + STAT, tokens), F32),
            pltpu.VMEM((k_out, tokens), F32),
            pltpu.VMEM((1, tokens), F32),
            pltpu.VMEM((rows, tokens), BF16),
            pltpu.SemaphoreType.DMA((3,)),
            pltpu.SemaphoreType.DMA((n_chunks,)),
            pltpu.SemaphoreType.DMA((n_chunks,)),
        ],
        name="local_pass",
    )(logits, labels, act, pin, pout)


def _join_kernel(*refs, k_in, k_out):
    parts, out = refs[:-1], refs[-1]
    base = k_in + 2 * k_out
    stats = [p[base : base + STAT, :].astype(F32) for p in parts]
    top = functools.reduce(jnp.maximum, [s[0:1] for s in stats])
    weights = [jnp.exp2((s[0:1] - top) * LOG2E) for s in stats]
    total = sum(w * (s[1:2] + s[2:3]) for w, s in zip(weights, stats))
    scale = 1.0 / total
    left = sum(p[0:k_in, :].astype(F32) for p in parts)
    right = sum(p[k_in : k_in + k_out, :].astype(F32) * w for p, w in zip(parts, weights)) * scale
    right = right - sum(p[k_in + k_out : base, :].astype(F32) for p in parts)
    out[0:k_in, :] = left.astype(BF16)
    out[k_in : k_in + k_out, :] = right.astype(BF16)


def _join(parts, k_in, k_out):
    return pl.pallas_call(
        functools.partial(_join_kernel, k_in=k_in, k_out=k_out),
        out_shape=pltpu.VMEM((k_in + k_out, parts[0].shape[1]), BF16),
        in_specs=[pl.BlockSpec(memory_space=pltpu.VMEM)] * len(parts),
        out_specs=pl.BlockSpec(memory_space=pltpu.VMEM),
        name="join",
    )(*_on_chip(parts))


def _gram_body(x, out_hbm, frow, fcol, res, sem, n_row, n_col, k_out):
    lanes = x.shape[2]
    base = n_row + n_col

    def feature_rows(first, count, dest, dest_first):
        for z in range(lanes // LANES):
            cols = slice(z * LANES, (z + 1) * LANES)
            for j in range(0, k_out, 16):
                rights = [x[t, base + j : base + j + 16, cols] for t in range(SEQ)]
                for i in range(count):
                    total = None
                    for t in range(SEQ):
                        term = x[t, first + i : first + i + 1, cols] * rights[t]
                        total = term if total is None else total + term
                    at = dest_first + i * k_out + j
                    dest[at : at + 16, cols] = total.astype(BF16)

    feature_rows(n_row, n_col, fcol, 0)
    step = max(1, n_row // 4)
    copies = []
    for b, i in enumerate(range(0, n_row, step)):
        feature_rows(i, step, frow, i * k_out)
        rows = slice(i * k_out, (i + step) * k_out)
        res[rows, :] = lax.dot_general(
            frow[rows, :], fcol[...], (((1,), (1,)), ((), ())), preferred_element_type=F32
        )
        c = pltpu.make_async_copy(res.at[rows, :], out_hbm.at[rows, :], sem.at[b])
        c.start()
        copies.append(c)
    for c in copies:
        c.wait()


def _gram_kernel(*refs, n_in, blocks, examples, n_row, n_col, k_in, k_out):
    ins, out_hbm = refs[:n_in], refs[n_in]
    x, frow, fcol, res, sem = refs[n_in + 1 :]
    rows = k_in + k_out
    half = n_in // 2
    if blocks:
        row_first = lax.axis_index("fsdp") * n_row
        col_first = lax.axis_index("dp") * n_col
        per = LANES // examples
        for k in range(half):
            for z in range(blocks):
                takes = [
                    (pl.ds(pl.multiple_of(z * rows + row_first, 8), n_row), 0, n_row),
                    (pl.ds(pl.multiple_of(z * rows + col_first, 8), n_col), n_row, n_col),
                    (slice(z * rows + k_in, (z + 1) * rows), n_row + n_col, k_out),
                ]
                for take, at, count in takes:
                    own = ins[k][take, :].astype(F32)
                    other = ins[half + k][take, :].astype(F32)
                    for s in range(per):
                        piece = slice(s * examples, (s + 1) * examples)
                        x[k * per + s, at : at + count, z * LANES : (z + 1) * LANES] = jnp.concatenate(
                            [own[:, piece], other[:, piece]], axis=1
                        )
    else:
        x[...] = ins[0][...].astype(F32)
    _gram_body(x, out_hbm, frow, fcol, res, sem, n_row, n_col, k_out)


def _gram(ins, blocks, examples, lanes, n_row, n_col, k_in, k_out):
    rows, cols = n_row * k_out, n_col * k_out
    return pl.pallas_call(
        functools.partial(
            _gram_kernel,
            n_in=len(ins),
            blocks=blocks,
            examples=examples,
            n_row=n_row,
            n_col=n_col,
            k_in=k_in,
            k_out=k_out,
        ),
        out_shape=jax.ShapeDtypeStruct((rows, cols), F32),
        in_specs=[pl.BlockSpec(memory_space=pltpu.VMEM)] * len(ins),
        out_specs=pl.BlockSpec(memory_space=pl.ANY),
        scratch_shapes=[
            pltpu.VMEM((SEQ, n_row + n_col + k_out, lanes), F32),
            pltpu.VMEM((rows, lanes), BF16),
            pltpu.VMEM((cols, lanes), BF16),
            pltpu.VMEM((rows, cols), F32),
            pltpu.SemaphoreType.DMA((8,)),
        ],
        name="gram",
    )(*_on_chip(ins))


def body(logits, labels, activations, proj_in, proj_out):
    n_f, n_d = lax.axis_size("fsdp"), lax.axis_size("dp")
    tokens = logits.shape[0]
    k_in, k_out = proj_in.shape[1], proj_out.shape[1]
    rows = k_in + k_out
    examples = tokens // SEQ
    own_examples = examples // n_f
    share = tokens // n_f

    def along_f(a, k):
        return lax.ppermute(a, "fsdp", [(i, _partner(i, k, n_f)) for i in range(n_f)])

    def along_z(a, k):
        return lax.ppermute(a, "dp", [(i, 2 * _partner(i // 2, k, n_d // 2) + i % 2) for i in range(n_d)])

    def far_first(n):
        return range(n - 1, 0, -1)

    def other_core(a):
        return lax.ppermute(a, "dp", [(i, i ^ 1) for i in range(n_d)])

    parts = _local(logits.T, labels.reshape(1, tokens), activations, proj_in.T, proj_out.T, n_f)
    parts = [parts[0]] + [along_f(parts[k], k) for k in far_first(n_f)]
    joined = _join(parts, k_in, k_out)
    n_z = n_d // 2
    column = jnp.concatenate([joined] + [along_z(joined, k) for k in far_first(n_z)], axis=0)
    own = [column] + [along_f(column, k) for k in far_first(n_f)]
    other = [other_core(a) for a in own]

    mine = lax.axis_index("fsdp")
    if share >= examples:
        slots = share // examples
        pieces = []
        for a in own:
            part = a[:rows].reshape(rows, slots, examples)
            pieces.append(lax.dynamic_slice_in_dim(part, mine * own_examples, own_examples, 2))
        group = jnp.concatenate(pieces, axis=1)
    else:
        order = [mine] + [_partner(mine, k, n_f) if n_f & (n_f - 1) == 0 else (mine - k) % n_f for k in far_first(n_f)]
        whole = jnp.zeros((n_f, rows, share), BF16)
        for k, a in enumerate(own):
            whole = lax.dynamic_update_slice(whole, a[:rows][None], (order[k], 0, 0))
        whole = whole.transpose(1, 0, 2).reshape(rows, SEQ, examples)
        group = lax.dynamic_slice_in_dim(whole, mine * own_examples, own_examples, 2)
    features = jnp.einsum("ite,jte->eij", group[:k_in], group[k_in:], preferred_element_type=F32)
    features = features.reshape(own_examples, k_in * k_out)

    n_row, n_col = k_in // n_f, k_in // n_d
    lanes = examples * n_d
    if share == LANES and 2 * examples == LANES and n_row % 8 == 0 and n_col % 8 == 0:
        gram = _gram(own + other, n_z, examples, lanes, n_row, n_col, k_in, k_out)
    else:
        order = [mine] + [_partner(mine, k, n_f) if n_f & (n_f - 1) == 0 else (mine - k) % n_f for k in far_first(n_f)]
        whole = jnp.zeros((n_f, 2, n_z, rows, share), BF16)
        for c, arrays in enumerate((own, other)):
            for k, a in enumerate(arrays):
                whole = lax.dynamic_update_slice(whole, a.reshape(1, 1, n_z, rows, share), (order[k], c, 0, 0, 0))
        whole = whole.transpose(3, 1, 2, 0, 4).reshape(rows, 2, n_z, SEQ, examples)
        whole = whole.transpose(3, 0, 1, 2, 4).reshape(SEQ, rows, lanes)
        whole = jnp.concatenate(
            [
                lax.dynamic_slice_in_dim(whole, mine * n_row, n_row, 1),
                lax.dynamic_slice_in_dim(whole, lax.axis_index("dp") * n_col, n_col, 1),
                whole[:, k_in:],
            ],
            axis=1,
        )
        gram = _gram([whole], 0, examples, lanes, n_row, n_col, k_in, k_out)
    return features, gram


def solution(mesh):
    in_specs = (P("dp", "fsdp"), P("dp"), P("dp", "fsdp"), P("fsdp", None), P("fsdp", None))
    out_specs = (P(("dp", "fsdp"), None), P("fsdp", "dp"))
    return jax.shard_map(body, mesh=mesh, in_specs=in_specs, out_specs=out_specs, check_vma=False)
```

```python
import functools

import jax
import jax.numpy as jnp
from jax import lax
from jax.experimental import pallas as pl
from jax.experimental.pallas import tpu as pltpu
from jax.sharding import PartitionSpec as P

SEQ = 8
LOG2E = 1.4426950408889634
LANES = 128
SHARES = (0.15, 0.35, 0.35, 1.0)
SUB = 256
STAT = 16
AHEAD = 20
F32 = jnp.float32
BF16 = jnp.bfloat16


def _cdiv(a, b):
    return (a + b - 1) // b


def _sizes(total, step, first=None):
    out = []
    start = 0
    while start < total:
        size = min(first if first and not start else step, total - start)
        out.append((start, size))
        start += size
    return out


def _plan(total):
    out, start = [], 0
    for share in SHARES:
        size = min(_cdiv(int(total * share), LANES) * LANES, total - start)
        if size > 0:
            out.append((start, size))
            start += size
    return out


def _partner(i, k, n):
    return i ^ k if n & (n - 1) == 0 else (i + k) % n


def _on_chip(arrays):
    return [pltpu.with_memory_space_constraint(a, pltpu.VMEM) for a in arrays]


def _local_kernel(
    logits_hbm, labels_hbm, act_hbm, pin_hbm, pout_hbm, *rest, groups, vocab, tokens, width, k_in, k_out
):
    outs = rest[:groups]
    buf, lab, act, pin, pext, wide, acc, plab, top, msg, sem, lsem, psem = rest[groups:]
    chunks = _plan(vocab)
    queue, loads, pout_loads = [], [], []
    label_load = pltpu.make_async_copy(labels_hbm, lab, sem.at[0])
    act_load = pltpu.make_async_copy(act_hbm, act, sem.at[1])
    pin_load = pltpu.make_async_copy(pin_hbm, pin, sem.at[2])
    for n, (start, size) in enumerate(chunks):
        cols = slice(start, start + size)
        loads.append(pltpu.make_async_copy(logits_hbm.at[cols, :], buf.at[cols, :], lsem.at[n]))
        pout_loads.append(pltpu.make_async_copy(pout_hbm.at[:, cols], pext.at[0:k_out, cols], psem.at[n]))
        queue.append((loads[n], pout_loads[n], label_load) if n == 0 else (loads[n], pout_loads[n]))
        if n == min(1, len(chunks) - 1):
            queue.append((act_load, pin_load))
    started = 0

    def start_next(count):
        nonlocal started
        for group in queue[started : started + count]:
            for c in group:
                c.start()
        started += count

    start_next(AHEAD)
    mine = lax.axis_index("fsdp")
    label_load.wait()
    pext[k_out : k_out + STAT, :] = jnp.ones((STAT, vocab), BF16)
    acc[...] = jnp.zeros_like(acc)
    plab[...] = jnp.zeros_like(plab)
    top[...] = jnp.full_like(top, -1e30)
    local = lab[...] - mine * vocab
    inside = (local >= 0) & (local < vocab)
    local = jnp.where(inside, local, -LANES)
    block = lax.shift_right_arithmetic(local, 7)
    lane = jnp.bitwise_and(local, LANES - 1)

    for n, (start, size) in enumerate(chunks):
        loads[n].wait()
        pout_loads[n].wait()
        start_next(1)
        if n == min(2, len(chunks) - 1):
            start_next(len(queue))
            act_load.wait()
            pin_load.wait()
            left = lax.dot_general(pin[...], act[...], (((1,), (1,)), ((), ())), preferred_element_type=F32)
            msg[0:k_in, :] = left.astype(BF16)
        peak = None
        for r, h in _sizes(size, 16):
            part = buf[start + r : start + r + h, :]
            peak = part if peak is None else jnp.maximum(peak, part)
        peak = jnp.max(peak.astype(F32), axis=0, keepdims=True)
        old = top[...]
        new = jnp.maximum(old, peak)
        top[...] = new
        keep = jnp.exp2((old - new) * LOG2E)
        total = acc[...] * keep
        for r, h in _sizes(size, SUB):
            part = buf[start + r : start + r + h, :].astype(F32)
            expo = jnp.exp2((part - new) * LOG2E).astype(BF16)
            total = total + jnp.dot(pext[:, start + r : start + r + h], expo, preferred_element_type=F32)
        acc[...] = total
        blocks = _sizes(size, LANES)
        for r, h in blocks:
            wide[:, r : r + h] = pext[0:k_out, start + r : start + r + h].astype(F32)
        for t in range(_cdiv(tokens, LANES)):
            cols = slice(t * LANES, (t + 1) * LANES)
            which = jnp.broadcast_to(block[:, cols], (k_out, LANES))
            index = jnp.broadcast_to(lane[:, cols], (k_out, LANES))
            found = plab[:, cols]
            for r, h in blocks:
                got = jnp.take_along_axis(wide[:, r : r + LANES], index, axis=1)
                found = jnp.where(which == (start + r) // LANES, got, found)
            plab[:, cols] = found

    msg[k_in : k_in + k_out, :] = acc[0:k_out, :].astype(BF16)
    msg[k_in + k_out : k_in + 2 * k_out, :] = plab[...].astype(BF16)
    sums = acc[k_out : k_out + STAT, :]
    high = sums.astype(BF16).astype(F32)
    row = lax.broadcasted_iota(jnp.int32, (STAT, tokens), 0)
    stat = jnp.where(row == 0, top[...], jnp.where(row == 1, high, jnp.where(row == 2, sums - high, 0.0)))
    msg[k_in + 2 * k_out :, :] = stat.astype(BF16)
    share = tokens // groups
    examples = tokens // SEQ
    src = lax.broadcasted_iota(jnp.int32, (tokens, share), 0)
    place = lax.broadcasted_iota(jnp.int32, (tokens, share), 1)
    for k in range(groups):
        dst = place + _partner(mine, k, groups) * share
        want = jnp.bitwise_and(dst, examples - 1) * SEQ + lax.shift_right_arithmetic(dst, examples.bit_length() - 1)
        pick = jnp.where(src == want, 1.0, 0.0).astype(BF16)
        outs[k][...] = jnp.dot(msg[...], pick, preferred_element_type=F32).astype(BF16)


def _local(logits, labels, act, pin, pout, groups):
    vocab, tokens = logits.shape
    k_in, width = pin.shape
    k_out = pout.shape[0]
    rows = k_in + 2 * k_out + STAT
    share = tokens // groups
    n_chunks = len(_plan(vocab))
    any_spec = pl.BlockSpec(memory_space=pl.ANY)
    return pl.pallas_call(
        functools.partial(
            _local_kernel, groups=groups, vocab=vocab, tokens=tokens, width=width, k_in=k_in, k_out=k_out
        ),
        out_shape=[pltpu.VMEM((rows, share), BF16)] * groups,
        in_specs=[any_spec] * 5,
        out_specs=[pl.BlockSpec(memory_space=pltpu.VMEM)] * groups,
        scratch_shapes=[
            pltpu.VMEM((vocab, tokens), BF16),
            pltpu.VMEM((1, tokens), jnp.int32),
            pltpu.VMEM((tokens, width), BF16),
            pltpu.VMEM((k_in, width), BF16),
            pltpu.VMEM((k_out + STAT, vocab), BF16),
            pltpu.VMEM((k_out, max(size for _, size in _plan(vocab)) + LANES), F32),
            pltpu.VMEM((k_out + STAT, tokens), F32),
            pltpu.VMEM((k_out, tokens), F32),
            pltpu.VMEM((1, tokens), F32),
            pltpu.VMEM((rows, tokens), BF16),
            pltpu.SemaphoreType.DMA((3,)),
            pltpu.SemaphoreType.DMA((n_chunks,)),
            pltpu.SemaphoreType.DMA((n_chunks,)),
        ],
        name="local_pass",
    )(logits, labels, act, pin, pout)


def _join_kernel(*refs, k_in, k_out):
    parts, out = refs[:-1], refs[-1]
    base = k_in + 2 * k_out
    stats = [p[base : base + STAT, :].astype(F32) for p in parts]
    top = functools.reduce(jnp.maximum, [s[0:1] for s in stats])
    weights = [jnp.exp2((s[0:1] - top) * LOG2E) for s in stats]
    total = sum(w * (s[1:2] + s[2:3]) for w, s in zip(weights, stats))
    scale = 1.0 / total
    left = sum(p[0:k_in, :].astype(F32) for p in parts)
    right = sum(p[k_in : k_in + k_out, :].astype(F32) * w for p, w in zip(parts, weights)) * scale
    right = right - sum(p[k_in + k_out : base, :].astype(F32) for p in parts)
    out[0:k_in, :] = left.astype(BF16)
    out[k_in : k_in + k_out, :] = right.astype(BF16)


def _join(parts, k_in, k_out):
    return pl.pallas_call(
        functools.partial(_join_kernel, k_in=k_in, k_out=k_out),
        out_shape=pltpu.VMEM((k_in + k_out, parts[0].shape[1]), BF16),
        in_specs=[pl.BlockSpec(memory_space=pltpu.VMEM)] * len(parts),
        out_specs=pl.BlockSpec(memory_space=pltpu.VMEM),
        name="join",
    )(*_on_chip(parts))


def _gram_body(x, out_hbm, frow, fcol, res, sem, n_row, n_col, k_out):
    lanes = x.shape[2]
    base = n_row + n_col

    def feature_rows(first, count, dest, dest_first):
        for z in range(lanes // LANES):
            cols = slice(z * LANES, (z + 1) * LANES)
            for j in range(0, k_out, 16):
                rights = [x[t, base + j : base + j + 16, cols] for t in range(SEQ)]
                for i in range(count):
                    total = None
                    for t in range(SEQ):
                        term = x[t, first + i : first + i + 1, cols] * rights[t]
                        total = term if total is None else total + term
                    at = dest_first + i * k_out + j
                    dest[at : at + 16, cols] = total.astype(BF16)

    feature_rows(n_row, n_col, fcol, 0)
    step = max(1, n_row // 4)
    copies = []
    for b, i in enumerate(range(0, n_row, step)):
        feature_rows(i, step, frow, i * k_out)
        rows = slice(i * k_out, (i + step) * k_out)
        res[rows, :] = lax.dot_general(
            frow[rows, :], fcol[...], (((1,), (1,)), ((), ())), preferred_element_type=F32
        )
        c = pltpu.make_async_copy(res.at[rows, :], out_hbm.at[rows, :], sem.at[b])
        c.start()
        copies.append(c)
    for c in copies:
        c.wait()


def _gram_kernel(*refs, n_in, blocks, examples, n_row, n_col, k_in, k_out):
    ins, out_hbm = refs[:n_in], refs[n_in]
    x, frow, fcol, res, sem = refs[n_in + 1 :]
    rows = k_in + k_out
    half = n_in // 2
    if blocks:
        row_first = lax.axis_index("fsdp") * n_row
        col_first = lax.axis_index("dp") * n_col
        per = LANES // examples
        for k in range(half):
            for z in range(blocks):
                takes = [
                    (pl.ds(pl.multiple_of(z * rows + row_first, 8), n_row), 0, n_row),
                    (pl.ds(pl.multiple_of(z * rows + col_first, 8), n_col), n_row, n_col),
                    (slice(z * rows + k_in, (z + 1) * rows), n_row + n_col, k_out),
                ]
                for take, at, count in takes:
                    own = ins[k][take, :].astype(F32)
                    other = ins[half + k][take, :].astype(F32)
                    for s in range(per):
                        piece = slice(s * examples, (s + 1) * examples)
                        x[k * per + s, at : at + count, z * LANES : (z + 1) * LANES] = jnp.concatenate(
                            [own[:, piece], other[:, piece]], axis=1
                        )
    else:
        x[...] = ins[0][...].astype(F32)
    _gram_body(x, out_hbm, frow, fcol, res, sem, n_row, n_col, k_out)


def _gram(ins, blocks, examples, lanes, n_row, n_col, k_in, k_out):
    rows, cols = n_row * k_out, n_col * k_out
    return pl.pallas_call(
        functools.partial(
            _gram_kernel,
            n_in=len(ins),
            blocks=blocks,
            examples=examples,
            n_row=n_row,
            n_col=n_col,
            k_in=k_in,
            k_out=k_out,
        ),
        out_shape=jax.ShapeDtypeStruct((rows, cols), F32),
        in_specs=[pl.BlockSpec(memory_space=pltpu.VMEM)] * len(ins),
        out_specs=pl.BlockSpec(memory_space=pl.ANY),
        scratch_shapes=[
            pltpu.VMEM((SEQ, n_row + n_col + k_out, lanes), F32),
            pltpu.VMEM((rows, lanes), BF16),
            pltpu.VMEM((cols, lanes), BF16),
            pltpu.VMEM((rows, cols), F32),
            pltpu.SemaphoreType.DMA((8,)),
        ],
        name="gram",
    )(*_on_chip(ins))


def _features_kernel(*refs, examples, own, k_in, k_out):
    ins, out, turned = refs[:-2], refs[-2], refs[-1]
    rows = k_in + k_out
    first = lax.axis_index("fsdp") * own
    parts = []
    for k, src in enumerate(ins):
        turned[k] = jnp.transpose(src[0:rows, :].astype(F32))
        for s in range(LANES // examples):
            parts.append(turned[k, pl.ds(pl.multiple_of(s * examples + first, 8), own), :])
    left = jnp.concatenate([p[:, :k_in] for p in parts], axis=0).astype(BF16)
    rights = [jnp.concatenate([p[:, k_in:], p[:, k_in:]], axis=1) for p in parts]
    width = 4 * LANES
    for n in range(0, k_in * k_out, width):
        row = lax.broadcasted_iota(jnp.int32, (k_in, width), 0)
        col = lax.broadcasted_iota(jnp.int32, (k_in, width), 1) + n
        spread = jnp.where((col >= row * k_out) & (col < (row + 1) * k_out), 1.0, 0.0).astype(BF16)
        wide = jnp.dot(left, spread, preferred_element_type=F32)
        for c in range(0, width, LANES):
            terms = [wide[t * own : (t + 1) * own, c : c + LANES] * r for t, r in enumerate(rights)]
            out[:, n + c : n + c + LANES] = functools.reduce(jnp.add, terms)


def _features(arrays, examples, own, k_in, k_out):
    return pl.pallas_call(
        functools.partial(_features_kernel, examples=examples, own=own, k_in=k_in, k_out=k_out),
        out_shape=pltpu.VMEM((own, k_in * k_out), F32),
        in_specs=[pl.BlockSpec(memory_space=pltpu.VMEM)] * len(arrays),
        out_specs=pl.BlockSpec(memory_space=pltpu.VMEM),
        scratch_shapes=[pltpu.VMEM((len(arrays), LANES, k_in + k_out), F32)],
        name="own_features",
    )(*_on_chip(arrays))


def body(logits, labels, activations, proj_in, proj_out):
    n_f, n_d = lax.axis_size("fsdp"), lax.axis_size("dp")
    tokens = logits.shape[0]
    k_in, k_out = proj_in.shape[1], proj_out.shape[1]
    rows = k_in + k_out
    examples = tokens // SEQ
    own_examples = examples // n_f
    share = tokens // n_f

    def along_f(a, k):
        return lax.ppermute(a, "fsdp", [(i, _partner(i, k, n_f)) for i in range(n_f)])

    def along_z(a, k):
        return lax.ppermute(a, "dp", [(i, 2 * _partner(i // 2, k, n_d // 2) + i % 2) for i in range(n_d)])

    def far_first(n):
        return range(n - 1, 0, -1)

    def other_core(a):
        return lax.ppermute(a, "dp", [(i, i ^ 1) for i in range(n_d)])

    parts = _local(logits.T, labels.reshape(1, tokens), activations, proj_in.T, proj_out.T, n_f)
    parts = [parts[0]] + [along_f(parts[k], k) for k in far_first(n_f)]
    joined = _join(parts, k_in, k_out)
    n_z = n_d // 2
    column = jnp.concatenate([joined] + [along_z(joined, k) for k in far_first(n_z)], axis=0)
    own = [column] + [along_f(column, k) for k in far_first(n_f)]
    other = [other_core(a) for a in own]

    mine = lax.axis_index("fsdp")
    group = None
    if share == LANES and 2 * k_out == LANES and k_in == k_out and own_examples % 8 == 0 and share % examples == 0:
        features = _features(own, examples, own_examples, k_in, k_out)
    elif share >= examples:
        slots = share // examples
        pieces = []
        for a in own:
            part = a[:rows].reshape(rows, slots, examples)
            pieces.append(lax.dynamic_slice_in_dim(part, mine * own_examples, own_examples, 2))
        group = jnp.concatenate(pieces, axis=1)
    else:
        order = [mine] + [_partner(mine, k, n_f) if n_f & (n_f - 1) == 0 else (mine - k) % n_f for k in far_first(n_f)]
        whole = jnp.zeros((n_f, rows, share), BF16)
        for k, a in enumerate(own):
            whole = lax.dynamic_update_slice(whole, a[:rows][None], (order[k], 0, 0))
        whole = whole.transpose(1, 0, 2).reshape(rows, SEQ, examples)
        group = lax.dynamic_slice_in_dim(whole, mine * own_examples, own_examples, 2)
    if group is not None:
        features = jnp.einsum("ite,jte->eij", group[:k_in], group[k_in:], preferred_element_type=F32)
        features = features.reshape(own_examples, k_in * k_out)

    n_row, n_col = k_in // n_f, k_in // n_d
    lanes = examples * n_d
    if share == LANES and 2 * examples == LANES and n_row % 8 == 0 and n_col % 8 == 0:
        gram = _gram(own + other, n_z, examples, lanes, n_row, n_col, k_in, k_out)
    else:
        order = [mine] + [_partner(mine, k, n_f) if n_f & (n_f - 1) == 0 else (mine - k) % n_f for k in far_first(n_f)]
        whole = jnp.zeros((n_f, 2, n_z, rows, share), BF16)
        for c, arrays in enumerate((own, other)):
            for k, a in enumerate(arrays):
                whole = lax.dynamic_update_slice(whole, a.reshape(1, 1, n_z, rows, share), (order[k], c, 0, 0, 0))
        whole = whole.transpose(3, 1, 2, 0, 4).reshape(rows, 2, n_z, SEQ, examples)
        whole = whole.transpose(3, 0, 1, 2, 4).reshape(SEQ, rows, lanes)
        whole = jnp.concatenate(
            [
                lax.dynamic_slice_in_dim(whole, mine * n_row, n_row, 1),
                lax.dynamic_slice_in_dim(whole, lax.axis_index("dp") * n_col, n_col, 1),
                whole[:, k_in:],
            ],
            axis=1,
        )
        gram = _gram([whole], 0, examples, lanes, n_row, n_col, k_in, k_out)
    return features, gram


def solution(mesh):
    in_specs = (P("dp", "fsdp"), P("dp"), P("dp", "fsdp"), P("fsdp", None), P("fsdp", None))
    out_specs = (P(("dp", "fsdp"), None), P("fsdp", "dp"))
    return jax.shard_map(body, mesh=mesh, in_specs=in_specs, out_specs=out_specs, check_vma=False)
```

```python
import functools

import jax
import jax.numpy as jnp
from jax import lax
from jax.experimental import pallas as pl
from jax.experimental.pallas import tpu as pltpu
from jax.sharding import PartitionSpec as P

SEQ = 8
LOG2E = 1.4426950408889634
LANES = 128
SHARES = (0.15, 0.35, 0.35, 1.0)
SUB = 256
STAT = 16
GROUPS = 4
AHEAD = 20
F32 = jnp.float32
BF16 = jnp.bfloat16


def _cdiv(a, b):
    return (a + b - 1) // b


def _sizes(total, step, first=None):
    out = []
    start = 0
    while start < total:
        size = min(first if first and not start else step, total - start)
        out.append((start, size))
        start += size
    return out


def _plan(total):
    out, start = [], 0
    for share in SHARES:
        size = min(_cdiv(int(total * share), LANES) * LANES, total - start)
        if size > 0:
            out.append((start, size))
            start += size
    return out


def _partner(i, k, n):
    return i ^ k if n & (n - 1) == 0 else (i + k) % n


def _on_chip(arrays):
    return [pltpu.with_memory_space_constraint(a, pltpu.VMEM) for a in arrays]


def _local_kernel(
    logits_hbm, labels_hbm, act_hbm, pin_hbm, pout_hbm, *rest, groups, vocab, tokens, width, k_in, k_out
):
    outs = rest[:groups]
    buf, lab, act, pin, pext, wide, acc, plab, top, msg, sem, lsem, psem = rest[groups:]
    chunks = _plan(vocab)
    queue, loads, pout_loads = [], [], []
    label_load = pltpu.make_async_copy(labels_hbm, lab, sem.at[0])
    act_load = pltpu.make_async_copy(act_hbm, act, sem.at[1])
    pin_load = pltpu.make_async_copy(pin_hbm, pin, sem.at[2])
    for n, (start, size) in enumerate(chunks):
        cols = slice(start, start + size)
        loads.append(pltpu.make_async_copy(logits_hbm.at[cols, :], buf.at[cols, :], lsem.at[n]))
        pout_loads.append(pltpu.make_async_copy(pout_hbm.at[:, cols], pext.at[0:k_out, cols], psem.at[n]))
        queue.append((loads[n], pout_loads[n], label_load) if n == 0 else (loads[n], pout_loads[n]))
        if n == min(1, len(chunks) - 1):
            queue.append((act_load, pin_load))
    started = 0

    def start_next(count):
        nonlocal started
        for group in queue[started : started + count]:
            for c in group:
                c.start()
        started += count

    start_next(AHEAD)
    mine = lax.axis_index("fsdp")
    label_load.wait()
    pext[k_out : k_out + STAT, :] = jnp.ones((STAT, vocab), BF16)
    acc[...] = jnp.zeros_like(acc)
    plab[...] = jnp.zeros_like(plab)
    top[...] = jnp.full_like(top, -1e30)
    local = lab[...] - mine * vocab
    inside = (local >= 0) & (local < vocab)
    local = jnp.where(inside, local, -LANES)
    block = lax.shift_right_arithmetic(local, 7)
    lane = jnp.bitwise_and(local, LANES - 1)

    for n, (start, size) in enumerate(chunks):
        loads[n].wait()
        pout_loads[n].wait()
        start_next(1)
        if n == min(2, len(chunks) - 1):
            start_next(len(queue))
            act_load.wait()
            pin_load.wait()
            left = lax.dot_general(pin[...], act[...], (((1,), (1,)), ((), ())), preferred_element_type=F32)
            msg[0:k_in, :] = left.astype(BF16)
        peak = None
        for r, h in _sizes(size, 16):
            part = buf[start + r : start + r + h, :]
            peak = part if peak is None else jnp.maximum(peak, part)
        peak = jnp.max(peak.astype(F32), axis=0, keepdims=True)
        old = top[...]
        new = jnp.maximum(old, peak)
        top[...] = new
        keep = jnp.exp2((old - new) * LOG2E)
        total = acc[...] * keep
        for r, h in _sizes(size, SUB):
            part = buf[start + r : start + r + h, :].astype(F32)
            expo = jnp.exp2((part - new) * LOG2E).astype(BF16)
            total = total + jnp.dot(pext[:, start + r : start + r + h], expo, preferred_element_type=F32)
        acc[...] = total
        blocks = _sizes(size, LANES)
        for r, h in blocks:
            wide[:, r : r + h] = pext[0:k_out, start + r : start + r + h].astype(F32)
        for t in range(_cdiv(tokens, LANES)):
            cols = slice(t * LANES, (t + 1) * LANES)
            which = jnp.broadcast_to(block[:, cols], (k_out, LANES))
            index = jnp.broadcast_to(lane[:, cols], (k_out, LANES))
            found = plab[:, cols]
            for r, h in blocks:
                got = jnp.take_along_axis(wide[:, r : r + LANES], index, axis=1)
                found = jnp.where(which == (start + r) // LANES, got, found)
            plab[:, cols] = found

    msg[k_in : k_in + k_out, :] = acc[0:k_out, :].astype(BF16)
    msg[k_in + k_out : k_in + 2 * k_out, :] = plab[...].astype(BF16)
    sums = acc[k_out : k_out + STAT, :]
    high = sums.astype(BF16).astype(F32)
    row = lax.broadcasted_iota(jnp.int32, (STAT, tokens), 0)
    stat = jnp.where(row == 0, top[...], jnp.where(row == 1, high, jnp.where(row == 2, sums - high, 0.0)))
    msg[k_in + 2 * k_out :, :] = stat.astype(BF16)
    share = tokens // groups
    examples = tokens // SEQ
    src = lax.broadcasted_iota(jnp.int32, (tokens, share), 0)
    place = lax.broadcasted_iota(jnp.int32, (tokens, share), 1)
    for k in range(groups):
        dst = place + _partner(mine, k, groups) * share
        want = jnp.bitwise_and(dst, examples - 1) * SEQ + lax.shift_right_arithmetic(dst, examples.bit_length() - 1)
        pick = jnp.where(src == want, 1.0, 0.0).astype(BF16)
        outs[k][...] = jnp.dot(msg[...], pick, preferred_element_type=F32).astype(BF16)


def _local(logits, labels, act, pin, pout, groups):
    vocab, tokens = logits.shape
    k_in, width = pin.shape
    k_out = pout.shape[0]
    rows = k_in + 2 * k_out + STAT
    share = tokens // groups
    n_chunks = len(_plan(vocab))
    any_spec = pl.BlockSpec(memory_space=pl.ANY)
    return pl.pallas_call(
        functools.partial(
            _local_kernel, groups=groups, vocab=vocab, tokens=tokens, width=width, k_in=k_in, k_out=k_out
        ),
        out_shape=[pltpu.VMEM((rows, share), BF16)] * groups,
        in_specs=[any_spec] * 5,
        out_specs=[pl.BlockSpec(memory_space=pltpu.VMEM)] * groups,
        scratch_shapes=[
            pltpu.VMEM((vocab, tokens), BF16),
            pltpu.VMEM((1, tokens), jnp.int32),
            pltpu.VMEM((tokens, width), BF16),
            pltpu.VMEM((k_in, width), BF16),
            pltpu.VMEM((k_out + STAT, vocab), BF16),
            pltpu.VMEM((k_out, max(size for _, size in _plan(vocab)) + LANES), F32),
            pltpu.VMEM((k_out + STAT, tokens), F32),
            pltpu.VMEM((k_out, tokens), F32),
            pltpu.VMEM((1, tokens), F32),
            pltpu.VMEM((rows, tokens), BF16),
            pltpu.SemaphoreType.DMA((3,)),
            pltpu.SemaphoreType.DMA((n_chunks,)),
            pltpu.SemaphoreType.DMA((n_chunks,)),
        ],
        name="local_pass",
    )(logits, labels, act, pin, pout)


def _join_kernel(*refs, k_in, k_out):
    parts, out = refs[:-1], refs[-1]
    base = k_in + 2 * k_out
    stats = [p[base : base + STAT, :].astype(F32) for p in parts]
    top = functools.reduce(jnp.maximum, [s[0:1] for s in stats])
    weights = [jnp.exp2((s[0:1] - top) * LOG2E) for s in stats]
    total = sum(w * (s[1:2] + s[2:3]) for w, s in zip(weights, stats))
    scale = 1.0 / total
    left = sum(p[0:k_in, :].astype(F32) for p in parts)
    right = sum(p[k_in : k_in + k_out, :].astype(F32) * w for p, w in zip(parts, weights)) * scale
    right = right - sum(p[k_in + k_out : base, :].astype(F32) for p in parts)
    out[0:k_in, :] = left.astype(BF16)
    out[k_in : k_in + k_out, :] = right.astype(BF16)


def _join(parts, k_in, k_out):
    return pl.pallas_call(
        functools.partial(_join_kernel, k_in=k_in, k_out=k_out),
        out_shape=pltpu.VMEM((k_in + k_out, parts[0].shape[1]), BF16),
        in_specs=[pl.BlockSpec(memory_space=pltpu.VMEM)] * len(parts),
        out_specs=pl.BlockSpec(memory_space=pltpu.VMEM),
        name="join",
    )(*_on_chip(parts))


def _gram_body(x, out_hbm, frow, fcol, res, sem, n_row, n_col, k_out):
    lanes = x.shape[2]
    base = n_row + n_col

    def feature_rows(first, count, dest, dest_first):
        for z in range(lanes // LANES):
            cols = slice(z * LANES, (z + 1) * LANES)
            for j in range(0, k_out, 16):
                rights = [x[t, base + j : base + j + 16, cols] for t in range(SEQ)]
                for i in range(count):
                    total = None
                    for t in range(SEQ):
                        term = x[t, first + i : first + i + 1, cols] * rights[t]
                        total = term if total is None else total + term
                    at = dest_first + i * k_out + j
                    dest[at : at + 16, cols] = total.astype(BF16)

    feature_rows(n_row, n_col, fcol, 0)
    step = max(1, n_row // GROUPS)
    copies = []
    for b, i in enumerate(range(0, n_row, step)):
        feature_rows(i, step, frow, i * k_out)
        rows = slice(i * k_out, (i + step) * k_out)
        res[rows, :] = lax.dot_general(
            frow[rows, :], fcol[...], (((1,), (1,)), ((), ())), preferred_element_type=F32
        )
        c = pltpu.make_async_copy(res.at[rows, :], out_hbm.at[rows, :], sem.at[b])
        c.start()
        copies.append(c)
    for c in copies:
        c.wait()


def _gram_kernel(*refs, n_in, blocks, examples, n_row, n_col, k_in, k_out):
    ins, feats = refs[:n_in], refs[n_in]
    out_hbm, feats_hbm, x, frow, fcol, res, sem = refs[n_in + 1 :]
    rows = k_in + k_out
    leave = pltpu.make_async_copy(feats, feats_hbm, sem.at[sem.shape[0] - 1])
    leave.start()
    half = n_in // 2
    if blocks:
        row_first = lax.axis_index("fsdp") * n_row
        col_first = lax.axis_index("dp") * n_col
        per = LANES // examples
        for k in range(half):
            for z in range(blocks):
                takes = [
                    (pl.ds(pl.multiple_of(z * rows + row_first, 8), n_row), 0, n_row),
                    (pl.ds(pl.multiple_of(z * rows + col_first, 8), n_col), n_row, n_col),
                    (slice(z * rows + k_in, (z + 1) * rows), n_row + n_col, k_out),
                ]
                for take, at, count in takes:
                    own = ins[k][take, :].astype(F32)
                    other = ins[half + k][take, :].astype(F32)
                    for s in range(per):
                        piece = slice(s * examples, (s + 1) * examples)
                        x[k * per + s, at : at + count, z * LANES : (z + 1) * LANES] = jnp.concatenate(
                            [own[:, piece], other[:, piece]], axis=1
                        )
    else:
        x[...] = ins[0][...].astype(F32)
    _gram_body(x, out_hbm, frow, fcol, res, sem, n_row, n_col, k_out)
    leave.wait()


def _gram(ins, feats, blocks, examples, lanes, n_row, n_col, k_in, k_out):
    rows, cols = n_row * k_out, n_col * k_out
    return pl.pallas_call(
        functools.partial(
            _gram_kernel,
            n_in=len(ins),
            blocks=blocks,
            examples=examples,
            n_row=n_row,
            n_col=n_col,
            k_in=k_in,
            k_out=k_out,
        ),
        out_shape=[jax.ShapeDtypeStruct((rows, cols), F32), jax.ShapeDtypeStruct(feats.shape, F32)],
        in_specs=[pl.BlockSpec(memory_space=pltpu.VMEM)] * (len(ins) + 1),
        out_specs=[pl.BlockSpec(memory_space=pltpu.HBM)] * 2,
        scratch_shapes=[
            pltpu.VMEM((SEQ, n_row + n_col + k_out, lanes), F32),
            pltpu.VMEM((rows, lanes), BF16),
            pltpu.VMEM((cols, lanes), BF16),
            pltpu.VMEM((rows, cols), F32),
            pltpu.SemaphoreType.DMA((GROUPS + 1,)),
        ],
        name="gram",
    )(*_on_chip(ins + [feats]))


def _features_kernel(*refs, examples, own, k_in, k_out):
    ins, out, turned = refs[:-2], refs[-2], refs[-1]
    rows = k_in + k_out
    first = lax.axis_index("fsdp") * own
    parts = []
    for k, src in enumerate(ins):
        turned[k] = jnp.transpose(src[0:rows, :].astype(F32))
        for s in range(LANES // examples):
            parts.append(turned[k, pl.ds(pl.multiple_of(s * examples + first, 8), own), :])
    left = jnp.concatenate([p[:, :k_in] for p in parts], axis=0).astype(BF16)
    rights = [jnp.concatenate([p[:, k_in:], p[:, k_in:]], axis=1) for p in parts]
    width = 4 * LANES
    for n in range(0, k_in * k_out, width):
        row = lax.broadcasted_iota(jnp.int32, (k_in, width), 0)
        col = lax.broadcasted_iota(jnp.int32, (k_in, width), 1) + n
        spread = jnp.where((col >= row * k_out) & (col < (row + 1) * k_out), 1.0, 0.0).astype(BF16)
        wide = jnp.dot(left, spread, preferred_element_type=F32)
        for c in range(0, width, LANES):
            terms = [wide[t * own : (t + 1) * own, c : c + LANES] * r for t, r in enumerate(rights)]
            out[:, n + c : n + c + LANES] = functools.reduce(jnp.add, terms)


def _features(arrays, examples, own, k_in, k_out):
    return pl.pallas_call(
        functools.partial(_features_kernel, examples=examples, own=own, k_in=k_in, k_out=k_out),
        out_shape=pltpu.VMEM((own, k_in * k_out), F32),
        in_specs=[pl.BlockSpec(memory_space=pltpu.VMEM)] * len(arrays),
        out_specs=pl.BlockSpec(memory_space=pltpu.VMEM),
        scratch_shapes=[pltpu.VMEM((len(arrays), LANES, k_in + k_out), F32)],
        name="own_features",
    )(*_on_chip(arrays))


def body(logits, labels, activations, proj_in, proj_out):
    n_f, n_d = lax.axis_size("fsdp"), lax.axis_size("dp")
    tokens = logits.shape[0]
    k_in, k_out = proj_in.shape[1], proj_out.shape[1]
    rows = k_in + k_out
    examples = tokens // SEQ
    own_examples = examples // n_f
    share = tokens // n_f

    def along_f(a, k):
        return lax.ppermute(a, "fsdp", [(i, _partner(i, k, n_f)) for i in range(n_f)])

    def along_z(a, k):
        return lax.ppermute(a, "dp", [(i, 2 * _partner(i // 2, k, n_d // 2) + i % 2) for i in range(n_d)])

    def far_first(n):
        return range(n - 1, 0, -1)

    def other_core(a):
        return lax.ppermute(a, "dp", [(i, i ^ 1) for i in range(n_d)])

    parts = _local(logits.T, labels.reshape(1, tokens), activations, proj_in.T, proj_out.T, n_f)
    parts = [parts[0]] + [along_f(parts[k], k) for k in far_first(n_f)]
    joined = _join(parts, k_in, k_out)
    n_z = n_d // 2
    column = jnp.concatenate([joined] + [along_z(joined, k) for k in range(1, n_z)], axis=0)
    own = [column] + [along_f(column, k) for k in range(1, n_f)]
    other = [other_core(a) for a in own]

    mine = lax.axis_index("fsdp")
    group = None
    if share == LANES and 2 * k_out == LANES and k_in == k_out and own_examples % 8 == 0 and share % examples == 0:
        features = _features(own, examples, own_examples, k_in, k_out)
    elif share >= examples:
        slots = share // examples
        pieces = []
        for a in own:
            part = a[:rows].reshape(rows, slots, examples)
            pieces.append(lax.dynamic_slice_in_dim(part, mine * own_examples, own_examples, 2))
        group = jnp.concatenate(pieces, axis=1)
    else:
        order = [mine] + [_partner(mine, k, n_f) if n_f & (n_f - 1) == 0 else (mine - k) % n_f for k in range(1, n_f)]
        whole = jnp.zeros((n_f, rows, share), BF16)
        for k, a in enumerate(own):
            whole = lax.dynamic_update_slice(whole, a[:rows][None], (order[k], 0, 0))
        whole = whole.transpose(1, 0, 2).reshape(rows, SEQ, examples)
        group = lax.dynamic_slice_in_dim(whole, mine * own_examples, own_examples, 2)
    if group is not None:
        features = jnp.einsum("ite,jte->eij", group[:k_in], group[k_in:], preferred_element_type=F32)
        features = features.reshape(own_examples, k_in * k_out)

    n_row, n_col = k_in // n_f, k_in // n_d
    lanes = examples * n_d
    if share == LANES and 2 * examples == LANES and n_row % 8 == 0 and n_col % 8 == 0:
        gram, features = _gram(own + other, features, n_z, examples, lanes, n_row, n_col, k_in, k_out)
    else:
        order = [mine] + [_partner(mine, k, n_f) if n_f & (n_f - 1) == 0 else (mine - k) % n_f for k in range(1, n_f)]
        whole = jnp.zeros((n_f, 2, n_z, rows, share), BF16)
        for c, arrays in enumerate((own, other)):
            for k, a in enumerate(arrays):
                whole = lax.dynamic_update_slice(whole, a.reshape(1, 1, n_z, rows, share), (order[k], c, 0, 0, 0))
        whole = whole.transpose(3, 1, 2, 0, 4).reshape(rows, 2, n_z, SEQ, examples)
        whole = whole.transpose(3, 0, 1, 2, 4).reshape(SEQ, rows, lanes)
        whole = jnp.concatenate(
            [
                lax.dynamic_slice_in_dim(whole, mine * n_row, n_row, 1),
                lax.dynamic_slice_in_dim(whole, lax.axis_index("dp") * n_col, n_col, 1),
                whole[:, k_in:],
            ],
            axis=1,
        )
        gram, features = _gram([whole], features, 0, examples, lanes, n_row, n_col, k_in, k_out)
    return features, gram


def solution(mesh):
    in_specs = (P("dp", "fsdp"), P("dp"), P("dp", "fsdp"), P("fsdp", None), P("fsdp", None))
    out_specs = (P(("dp", "fsdp"), None), P("fsdp", "dp"))
    return jax.shard_map(body, mesh=mesh, in_specs=in_specs, out_specs=out_specs, check_vma=False)
```
